32 devices in a mesh: member: 2 (over core), tile: 16 (over z, y, x).
Axes of the slice: x: 2, y: 2, z: 4, core: 2. Of those that a mesh axis runs over, the one named last changes fastest.
Arguments:
- ensemble: bfloat16 [40, 7, 32, 2048], P('member', None, None, 'tile'), may hold values from -6 to 6
- control: bfloat16 [40, 32, 2048], P('member', None, 'tile'), may hold values from -6 to 6
- vert_loc: bfloat16 [32, 32], replicated, may hold values from -1 to 1
- obs_source: int32 [8192, 1], P('tile'), may hold values from 0 to 15; in each aligned block of 512 rows (0 to 511, 512 to 1023, ...) at most 64 rows name the same one
- obs_column: int32 [8192], P('tile'), may hold values from 0 to 127
- obs_slot: int32 [8192], P('tile'), may hold values from 0 to 5
- obs_frac: float32 [8192], P('tile'), may hold values from 0 to 1
- obs_count: int32 [16], P('tile'), may hold values from 1 to 512, 4096 in all
Outputs:
- obs_increment: float32 [32, 8192], P(None, 'tile')
The draws below stay inside these ranges and needn't reach their ends.
Inputs may be any that keep to these rules, and one draw needn't show every extreme that they name: `obs_source`: among the 512 observation slots of one owner tile, at most 64 name the same source tile, and some source tile is named exactly 64 times. `obs_count`: the counts sum to 4096 and one of them is 512.
All inputs are finite; a program needn't handle non-finite values. No bound on the sum of `obs_count` on one device may be relied on, other than what follows from the above.
Results may differ from the reference program's by a relative error of at most 0.0003.
Values sent between devices are 32-bit elements; how exact they have to be, the bound alone decides.
No kernel may reach another device: no remote copies, remote signals or barrier semaphores. Data moves between devices by JAX's collectives and lax.ppermute only.
A program may use at most 64 MiB of HBM per device.

```python
import math
import jax
import jax.numpy as jnp
import numpy as np
from jax import lax

MEM = 40
SLOTS = 7
LEV = 32
COL_DEV = 128
OBS_DEV = 512
COLS = 2048
OBS = 8192
CAP = 64
N_TILE = 16


def set_ends(result, own_key, low, largest):
    place = [jax.random.randint(jax.random.fold_in(own_key, axis), (), 0, length) for axis, length in enumerate(result.shape)]
    widest = result.shape.index(max(result.shape))
    neighbour = place[:widest] + [(place[widest] + 1) % result.shape[widest]] + place[widest + 1:]
    return result.at[tuple(place)].set(low).at[tuple(neighbour)].set(largest)


def level_of(key, shape, shards, low, largest):
    level = 1.0
    for axis_at, shards_of in shards:
        draws = jax.random.uniform(jax.random.fold_in(jax.random.fold_in(key, 6), axis_at), (shards_of,), jnp.float32, low / len(shards), largest / len(shards))
        level = level * jnp.repeat(jnp.exp(draws), shape[axis_at] // shards_of).reshape((-1,) + (1,) * (len(shape) - 1 - axis_at))
    return level


def split_up(number_of, total, limit, skew):
    portions = [(1 << 20) // math.isqrt(standing ** skew) + 1 for standing in range(2, number_of + 1)]
    spare, given = total - limit - (number_of - 1), [1] * (number_of - 1)
    while spare > 0:
        free = [i for i in range(number_of - 1) if given[i] < limit]
        mass, left = sum([portions[i] for i in free]), spare
        for i in free:
            extra = min(limit - given[i], max(1, left * portions[i] // mass), spare)
            given[i] = given[i] + extra
            spare = spare - extra
    return np.array([limit] + given)


def ragged(rng, count, total, limit, skew):
    if count == 2:
        one = jax.random.randint(rng, (), max(1, total - limit), min(limit, total - 1) + 1)
        return jnp.stack([one, total - one])
    lengths = jnp.asarray(split_up(count, total, limit, skew), jnp.int32)
    couples = (count - 1) // 2
    donor, taker = lengths[1:1 + 2 * couples:2], lengths[2:2 + 2 * couples:2]
    room = jnp.minimum(donor - 1, limit - taker)
    passed = jax.random.randint(jax.random.fold_in(rng, 1), (couples,), 0, 1 << 20) % (room + 1)
    lengths = lengths.at[1:1 + 2 * couples:2].set(donor - passed).at[2:2 + 2 * couples:2].set(taker + passed)
    return lengths[jax.random.permutation(jax.random.fold_in(rng, 2), count)]


def deal_out(rng, own, number, rows, number_of, top, limit, slope):
    order = jax.random.permutation(rng, number_of)
    crowded, common = load_shares(number_of, rows * top, limit, slope, True), load_shares(number_of, rows * top, limit, slope, False)
    places = jnp.arange(number_of)

    def named(sizes, turn):
        used = int((sizes > 0).sum())
        fixed = max(1, used // 4)
        shifted = fixed + (places - fixed + turn * (used - fixed)) % max(1, number_of - fixed)
        return jnp.zeros((number_of,), jnp.int32).at[order[jnp.where(places < fixed, places, shifted)]].set(jnp.asarray(sizes, jnp.int32))

    sizes = jnp.where(number % 4 == 0, named(crowded, number // 4), named(common, number - number // 4 - 1))
    mixed = jax.random.permutation(jax.random.fold_in(own, 3), number_of)
    giver, sink = mixed[0:number_of // 2 * 2:2], mixed[1:number_of // 2 * 2:2]
    slack = jnp.minimum(sizes[giver] - 1, limit - sizes[sink]) // 2
    slack = jnp.where((giver == order[0]) | (sink == order[0]) | (sizes[sink] == 0), 0, jnp.maximum(slack, 0))
    shifted = jax.random.randint(jax.random.fold_in(own, 4), (number_of // 2,), 0, 1 << 20) % (slack + 1)
    sizes = sizes.at[giver].add(-shifted).at[sink].add(shifted)
    items = jnp.searchsorted(jnp.cumsum(sizes), jnp.arange(rows * top), side="right").astype(jnp.int32)
    listing = items.reshape(top, rows).T
    listing = listing[jax.random.permutation(jax.random.fold_in(own, 1), rows)]
    turn = jax.random.randint(jax.random.fold_in(own, 2), (rows, 1), 0, top)
    return jnp.take_along_axis(listing, (jnp.arange(top)[None, :] + turn) % top, axis=1)


def load_shares(amount, total, most, slope, full):
    loads = [(1 << 20) // math.isqrt(standing ** slope) + 1 for standing in range(1, amount + 1)]
    largest = most if full else min(most, max(-(-total // amount), total * loads[0] // sum(loads)))
    least = 1 if total - largest >= amount - 1 else 0
    given, surplus = [largest] + [least] * (amount - 1), total - largest - least * (amount - 1)
    while surplus > 0:
        movable = [i for i in range(1, amount) if given[i] < largest] or [i for i in range(1, amount) if given[i] < most]
        pool, budget = sum([loads[i] for i in movable]), surplus
        for i in movable:
            more = min(most - given[i], max(1, budget * loads[i] // pool), surplus)
            given[i] = given[i] + more
            surplus = surplus - more
    return np.array(given)


def scatter_about(key, shape, scale, reach, pieces=(), held_as=jnp.bfloat16):
    level = level_of(key, shape, pieces, -0.22, 0.18) if pieces else 1.0
    entries = jax.random.normal(key, shape, jnp.float32) * scale * level
    return jnp.minimum(jnp.maximum(entries, -reach), reach).astype(held_as)


def setup_inputs(seed: int = 0) -> dict:
    key_of = jax.random.split(jax.random.key(seed), 9)
    ensemble = scatter_about(key_of[0], (MEM, SLOTS, LEV, COLS), 1.0, 6.0, ((0, 2), (3, 16)))
    control = scatter_about(key_of[1], (MEM, LEV, COLS), 1.0, 6.0, ((0, 2), (2, 16)))
    vert_loc = scatter_about(key_of[2], (LEV, LEV), LEV ** -0.5, 1.0)
    obs_source_keys = jax.random.split(jax.random.fold_in(key_of[3], 1), OBS // OBS_DEV)
    obs_source_turns = jax.random.permutation(jax.random.fold_in(key_of[3], 3), OBS // OBS_DEV)
    obs_source = jax.vmap(lambda own, number: deal_out(jax.random.fold_in(key_of[3], 2), own, number, OBS_DEV, N_TILE, 1, CAP, 2))(obs_source_keys, obs_source_turns).reshape((OBS, 1))
    obs_column = set_ends(jax.random.randint(key_of[4], (OBS,), 0, COL_DEV), jax.random.fold_in(key_of[4], 1), 0, COL_DEV - 1).astype(jnp.int32)
    obs_slot = set_ends(jax.random.randint(key_of[5], (OBS,), 0, SLOTS - 1), jax.random.fold_in(key_of[5], 1), 0, (SLOTS - 1) - 1).astype(jnp.int32)
    obs_frac = jnp.clip(1.0 * jax.random.uniform(key_of[6], (OBS,), jnp.float32) ** level_of(key_of[6], (OBS,), ((0, 16),), -0.2, 0.2), 0.0, 1.0)
    obs_count = ragged(key_of[7], N_TILE, OBS // 2, OBS_DEV, 2).astype(jnp.int32)
    return dict(ensemble=ensemble, control=control, vert_loc=vert_loc, obs_source=obs_source, obs_column=obs_column, obs_slot=obs_slot, obs_frac=obs_frac, obs_count=obs_count)


def reference(ensemble, control, vert_loc, obs_source, obs_column, obs_slot, obs_frac, obs_count):
    loc_float = vert_loc.astype(jnp.float32)

    def member_step(total, pair):
        member, ctrl = pair
        weighted = jnp.dot(loc_float, ctrl.astype(jnp.float32), precision=lax.Precision.HIGHEST)
        return total + member.astype(jnp.float32) * weighted[None], None

    start = jnp.zeros((SLOTS, LEV, COLS), jnp.float32)
    increment, _ = lax.scan(member_step, start, (ensemble, control))
    glob = (obs_source[:, 0] * COL_DEV + obs_column).astype(jnp.int32)
    lower = increment[obs_slot, :, glob].T
    upper = increment[obs_slot + 1, :, glob].T
    frac = obs_frac[None, :]
    value = (1.0 - frac) * lower + frac * upper
    live = (jnp.arange(OBS, dtype=jnp.int32) % OBS_DEV) < jnp.repeat(obs_count, OBS_DEV)
    return jnp.where(live[None, :], value, jnp.float32(0.0))
```

```python
import functools
import jax
import jax.numpy as jnp
from jax import lax
from jax.experimental import pallas as pl
from jax.experimental.pallas import tpu as pltpu
from jax.sharding import PartitionSpec as P

VMEM = pl.BlockSpec(memory_space=pltpu.VMEM)


def swap(value, axis, bits):
    return lax.ppermute(value, axis, [(i, i ^ bits) for i in range(lax.axis_size(axis))])


def partial_kernel(ensemble, control, vert_loc, *refs):
    *shares, total = refs
    group = lax.axis_index("member")
    rows = total.shape[1] // len(shares)
    total[...] = jnp.zeros_like(total)

    def member(k, carry):
        weighted = jnp.dot(vert_loc[...], control[k], preferred_element_type=jnp.float32)
        total[...] += ensemble[k].astype(jnp.float32) * weighted[None]
        return carry

    lax.fori_loop(0, ensemble.shape[0], member, 0, unroll=4)
    for j, share in enumerate(shares):
        first = pl.multiple_of((group ^ j) * rows, rows)
        share[...] = total[:, pl.ds(first, rows), :]


def pick_kernel(near, owners, *refs):
    blocks, metas = refs[:near], refs[near : near + owners]
    values, (high, low) = refs[near + owners : -2], refs[-2:]
    tile = lax.axis_index("tile")
    slots, levels, columns = blocks[0].shape
    rows = slots * levels
    for j, block in enumerate(blocks):
        part = block[...].reshape(rows, columns)
        top = part.astype(jnp.bfloat16)
        high[:, j * columns : (j + 1) * columns] = top
        low[:, j * columns : (j + 1) * columns] = (part - top.astype(jnp.float32)).astype(jnp.bfloat16)
    for meta, value in zip(metas, values, strict=True):
        source = meta[0:1, :].astype(jnp.int32)
        column = meta[1:2, :].astype(jnp.int32)
        slot = meta[2:3, :].astype(jnp.int32)
        frac = meta[3:4, :]
        relative = source ^ tile
        key = jnp.where((relative >= 0) & (relative < near), relative * columns + column, -1)
        place = lax.broadcasted_iota(jnp.int32, (near * columns, key.shape[1]), 0)
        hot = (place == key).astype(jnp.float32).astype(jnp.bfloat16)
        found = jnp.dot(high[...], hot, preferred_element_type=jnp.float32) + jnp.dot(
            low[...], hot, preferred_element_type=jnp.float32
        )
        found = found.reshape(slots, levels, key.shape[1])
        total = jnp.zeros_like(found[0])
        for t in range(slots):
            weight = jnp.where(slot == t, 1.0 - frac, jnp.where(slot + 1 == t, frac, 0.0))
            total += weight * found[t]
        value[...] = total


def join_kernel(*refs):
    *parts, out = refs
    group = lax.axis_index("member")
    rows = parts[0].shape[0]
    for j, part in enumerate(parts):
        out[pl.ds(pl.multiple_of((group ^ j) * rows, rows), rows), :] = part[...]


def on_device(ensemble, control, vert_loc, obs_source, obs_column, obs_slot, obs_frac, obs_count):
    groups, tiles = lax.axis_size("member"), lax.axis_size("tile")
    near = min(4, tiles)
    far = tiles // near
    members, slots, levels, columns = ensemble.shape
    obs = obs_column.shape[0]
    share = levels // groups

    live = jnp.arange(obs, dtype=jnp.int32) < obs_count[0]
    source = jnp.where(live, obs_source[:, 0], -1)
    meta = jnp.stack(
        [source.astype(jnp.float32), obs_column.astype(jnp.float32), obs_slot.astype(jnp.float32), obs_frac]
    )
    metas = [meta] + [swap(meta, "tile", j * near) for j in range(1, far)]

    shares = pl.pallas_call(
        partial_kernel,
        out_shape=[jax.ShapeDtypeStruct((slots, share, columns), jnp.float32)] * groups,
        in_specs=[VMEM] * 3,
        out_specs=[VMEM] * groups,
        scratch_shapes=[pltpu.VMEM((slots, levels, columns), jnp.float32)],
    )(ensemble, control, vert_loc)
    increment = shares[0]
    for j in range(1, groups):
        increment = increment + swap(shares[j], "member", j)

    blocks = [increment] + [swap(increment, "tile", j) for j in range(1, near)]
    values = pl.pallas_call(
        functools.partial(pick_kernel, near, far),
        out_shape=[jax.ShapeDtypeStruct((share, obs), jnp.float32)] * far,
        in_specs=[VMEM] * (near + far),
        out_specs=[VMEM] * far,
        scratch_shapes=[pltpu.VMEM((slots * share, near * columns), jnp.bfloat16)] * 2,
    )(*blocks, *metas)
    value = values[0]
    for j in range(1, far):
        value = value + swap(values[j], "tile", j * near)
    parts = [value] + [swap(value, "member", j) for j in range(1, groups)]
    return pl.pallas_call(
        join_kernel,
        out_shape=jax.ShapeDtypeStruct((levels, obs), jnp.float32),
        in_specs=[VMEM] * groups,
        out_specs=VMEM,
    )(*parts)


def solution(mesh):
    placed = (
        P("member", None, None, "tile"),
        P("member", None, "tile"),
        P(),
        P("tile", None),
        P("tile"),
        P("tile"),
        P("tile"),
        P("tile"),
    )
    return jax.shard_map(
        on_device, mesh=mesh, in_specs=placed, out_specs=P(None, "tile"), check_vma=False
    )
```
